32 devices in a mesh: worker: 8 (over y, x, core), mp: 4 (over z).
Axes of the slice: x: 2, y: 2, z: 4, core: 2. Of those that a mesh axis runs over, the one named last changes fastest.
Arguments:
- gradients: float32 [8, 2097152], P('worker', 'mp'), may hold values from -100 to 100
- neighbours: int32 [8, 3], replicated, may hold values from 0 to 7, as said below
- winner: int32 [1], replicated, may hold values from 0 to 7
Outputs:
- scores: float32 [8], replicated
- aggregate: float32 [2097152], P(('mp', 'worker'))
The draws below stay inside these ranges and needn't reach their ends.
Inputs may be any that keep to these rules, and one draw needn't show every extreme that they name: `neighbours`: row i lists 3 different workers, none of them equal to i.
All inputs are finite; a program needn't handle non-finite values.
Results may differ from the reference program's by a relative error of at most 0.0003.
Values may be sent and summed in bfloat16 or wider, within the bound.
No kernel may reach another device: no remote copies, remote signals or barrier semaphores. Data moves between devices by JAX's collectives and lax.ppermute only.
A program may use at most 64 MiB of HBM per device.

```python
import math
import jax
import jax.numpy as jnp
from jax import lax

FAULTY = 3
WORKERS = 8
NBR = 3
PARAMS = 2097152


def draw_gradients(key, part):
    keys = jax.random.split(jax.random.fold_in(key, 11), 10)
    noise = jnp.clip(jax.random.normal(keys[0], (WORKERS, PARAMS), jnp.float32), -6.0, 6.0)
    position = jnp.arange(PARAMS, dtype=jnp.float32) / jnp.float32(PARAMS)
    scales = jnp.exp(jax.random.uniform(keys[1], (WORKERS, 1), jnp.float32, math.log(0.5), math.log(2.0)))
    column = 0.5 * jnp.exp(math.log(3.0) * position)[None, :]
    values = scales * column * noise
    loadings = jax.random.uniform(keys[8], (WORKERS, 4), jnp.float32, -1.0, 1.0)
    shared = jnp.clip(jax.random.normal(keys[9], (4, PARAMS), jnp.float32), -6.0, 6.0)
    for factor in range(4):
        values = values + column * loadings[:, factor:factor + 1] * shared[factor][None, :]
    ranking = jax.random.permutation(keys[4], WORKERS)
    faulty = (ranking < FAULTY).astype(jnp.float32)[:, None]
    sparse = (jax.random.uniform(keys[5], (WORKERS, PARAMS), jnp.float32) < 1.0 / 4096.0).astype(jnp.float32)
    size = jax.random.uniform(keys[6], (WORKERS, PARAMS), jnp.float32, 20.0, 40.0)
    sign = jnp.where(jax.random.uniform(keys[7], (WORKERS, PARAMS), jnp.float32) < 0.5, -1.0, 1.0)
    values = values + faulty * sparse * sign * size * column
    return jnp.clip(values, -100.0, 100.0).astype(jnp.float32)


def draw_neighbours(key, part):
    keys = jax.random.split(jax.random.fold_in(key, 23), WORKERS)
    orders = jax.vmap(lambda single: jax.random.permutation(single, WORKERS - 1))(keys)[:, :NBR]
    orders = orders.astype(jnp.int32)
    own_index = jnp.arange(WORKERS, dtype=jnp.int32)[:, None]
    return (orders + (orders >= own_index).astype(jnp.int32)).astype(jnp.int32)


def setup_inputs(seed: int = 0) -> dict:
    streams_of = jax.random.split(jax.random.key(seed), 4)
    return {
        "gradients": draw_gradients(jax.random.fold_in(streams_of[3], 71), 0),
        "neighbours": draw_neighbours(jax.random.fold_in(streams_of[3], 71), 0),
        "winner": jax.random.randint(streams_of[2], (1,), 0, WORKERS).astype(jnp.int32),
    }


def reference(gradients, neighbours, winner):
    rounded = gradients.astype(jnp.bfloat16)
    gram_matrix = jnp.dot(rounded, rounded.T, preferred_element_type=jnp.float32)
    squares = jnp.diagonal(gram_matrix)
    distance = squares[:, None] + squares[None, :] - 2.0 * gram_matrix
    chosen = jnp.take_along_axis(distance, neighbours, axis=1)
    scores = jnp.sum(chosen, axis=1) / jnp.float32(NBR * PARAMS)
    aggregate = lax.dynamic_index_in_dim(gradients, winner[0], 0, keepdims=False)
    return (scores, aggregate)
```

```python
import jax
import jax.numpy as jnp
from jax import lax
from jax.experimental import pallas as pl
from jax.experimental.pallas import tpu as pltpu
from jax.sharding import PartitionSpec as P

LANES = 128


def score_kernel(neighbours, columns, out, *, scale):
    workers, rows, lanes = columns.shape
    nbr = neighbours.shape[1]
    chunk = 16

    def step(r, accs):
        at = pl.ds(pl.multiple_of(r * chunk, chunk), chunk)
        new = []
        for i in range(workers):
            own = columns[i, at, :].astype(jnp.float32)
            acc = accs[i]
            for j in range(nbr):
                diff = own - columns[neighbours[i, j], at, :].astype(jnp.float32)
                square = diff * diff
                acc = acc + (square[:8] + square[8:])
            new.append(acc)
        return tuple(new)

    zero = jnp.zeros((8, lanes), jnp.float32)
    accs = lax.fori_loop(0, rows // chunk, step, (zero,) * workers)
    lane = lax.broadcasted_iota(jnp.int32, (1, lanes), 1)
    row = jnp.zeros((1, lanes), jnp.float32)
    for i in range(workers):
        total = jnp.sum(jnp.sum(accs[i], axis=0, keepdims=True), axis=1, keepdims=True)
        row = jnp.where(lane == i, total * scale, row)
    out[...] = jnp.broadcast_to(row[None], out.shape)


def partial_scores(neighbours, columns, devices, scale):
    def kernel(n, c, o):
        score_kernel(n, c, o, scale=scale)

    return pl.pallas_call(
        kernel,
        out_shape=jax.ShapeDtypeStruct((devices, 1, LANES), jnp.float32),
        in_specs=[
            pl.BlockSpec(memory_space=pltpu.SMEM),
            pl.BlockSpec(memory_space=pltpu.VMEM),
        ],
        out_specs=pl.BlockSpec(memory_space=pltpu.VMEM),
        name="scores",
    )(neighbours, columns)


def low_part(x):
    return (x - lax.reduce_precision(x, 8, 7)).astype(jnp.bfloat16)


def body(gradients, neighbours, winner):
    workers = lax.axis_size("worker")
    devices = workers * lax.axis_size("mp")
    me = lax.axis_index("worker")
    length = gradients.shape[1]
    rows = length // workers // LANES
    pieces = gradients.reshape(workers, rows, LANES)
    columns = lax.all_to_all(
        pieces.astype(jnp.bfloat16), "worker", split_axis=0, concat_axis=0, tiled=True
    )
    scale = 1.0 / float(neighbours.shape[1] * length * lax.axis_size("mp"))
    partial_value = partial_scores(neighbours, columns, devices, scale)
    everyone = lax.all_to_all(
        partial_value, ("worker", "mp"), split_axis=0, concat_axis=0, tiled=True
    )
    scores = jnp.sum(everyone, axis=0)[0, :workers]

    chips = workers // 2
    chip, core = me // 2, me % 2
    best = winner[0]
    halves = pieces.reshape(chips, 2, rows, LANES)
    keep = lax.dynamic_index_in_dim(halves, core, 1, keepdims=False)
    give = lax.dynamic_index_in_dim(halves, 1 - core, 1, keepdims=False)
    got = lax.ppermute(low_part(give), "worker", [(i, i ^ 1) for i in range(workers)])
    mine = jnp.where(best % 2 == core, low_part(keep), got)
    low = lax.dynamic_index_in_dim(mine, chip, 0, keepdims=False)
    for d in range(1, chips):
        sent = lax.dynamic_index_in_dim(mine, chip ^ d, 0, keepdims=False)
        came = lax.ppermute(sent, "worker", [(i, i ^ (2 * d)) for i in range(workers)])
        low = jnp.where(best // 2 == chip ^ d, came, low)
    high = lax.dynamic_index_in_dim(columns, best, 0, keepdims=False)
    aggregate = high.astype(jnp.float32) + low.astype(jnp.float32)
    return (scores, aggregate.reshape(-1))


def solution(mesh):
    in_specs = (P("worker", "mp"), P(), P())
    out_specs = (P(), P(("mp", "worker")))
    return jax.shard_map(body, mesh=mesh, in_specs=in_specs, out_specs=out_specs, check_vma=False)
```

```python
import jax
import jax.numpy as jnp
from jax import lax
from jax.experimental import pallas as pl
from jax.experimental.pallas import tpu as pltpu
from jax.sharding import PartitionSpec as P

LANES = 128


def score_kernel(neighbours, columns, out, *, scale):
    workers, rows, lanes = columns.shape
    nbr = neighbours.shape[1]
    chunk = 16

    def step(r, accs):
        at = pl.ds(pl.multiple_of(r * chunk, chunk), chunk)
        new = []
        for i in range(workers):
            own = columns[i, at, :].astype(jnp.float32)
            acc = accs[i]
            for j in range(nbr):
                diff = own - columns[neighbours[i, j], at, :].astype(jnp.float32)
                square = diff * diff
                acc = acc + (square[:8] + square[8:])
            new.append(acc)
        return tuple(new)

    zero = jnp.zeros((8, lanes), jnp.float32)
    accs = lax.fori_loop(0, rows // chunk, step, (zero,) * workers)
    lane = lax.broadcasted_iota(jnp.int32, (1, lanes), 1)
    row = jnp.zeros((1, lanes), jnp.float32)
    for i in range(workers):
        total = jnp.sum(jnp.sum(accs[i], axis=0, keepdims=True), axis=1, keepdims=True)
        row = jnp.where(lane == i, total * scale, row)
    out[...] = jnp.broadcast_to(row[None], out.shape)


def partial_scores(neighbours, columns, devices, scale):
    def kernel(n, c, o):
        score_kernel(n, c, o, scale=scale)

    return pl.pallas_call(
        kernel,
        out_shape=jax.ShapeDtypeStruct((devices, 1, LANES), jnp.float32),
        in_specs=[
            pl.BlockSpec(memory_space=pltpu.SMEM),
            pl.BlockSpec(memory_space=pltpu.VMEM),
        ],
        out_specs=pl.BlockSpec(memory_space=pltpu.VMEM),
        name="scores",
    )(neighbours, columns)


def split_kernel(core, pieces, high, give, keep):
    value = pieces[0]
    rounded = value.astype(jnp.bfloat16)
    high[0] = rounded
    low = (value - rounded.astype(jnp.float32)).astype(jnp.bfloat16)
    mine = core[0] == pl.program_id(0) % 2

    @pl.when(mine)
    def _():
        keep[0] = low

    @pl.when(jnp.logical_not(mine))
    def _():
        give[0] = low


def split(core, pieces):
    workers, rows, lanes = pieces.shape
    block = (1, rows, lanes)
    half = jax.ShapeDtypeStruct((workers // 2, rows, lanes), jnp.bfloat16)
    return pl.pallas_call(
        split_kernel,
        grid=(workers,),
        out_shape=(jax.ShapeDtypeStruct(pieces.shape, jnp.bfloat16), half, half),
        in_specs=[
            pl.BlockSpec(memory_space=pltpu.SMEM),
            pl.BlockSpec(block, lambda i: (i, 0, 0)),
        ],
        out_specs=(
            pl.BlockSpec(block, lambda i: (i, 0, 0)),
            pl.BlockSpec(block, lambda i: (i // 2, 0, 0)),
            pl.BlockSpec(block, lambda i: (i // 2, 0, 0)),
        ),
        name="split",
    )(core, pieces)


def body(gradients, neighbours, winner):
    workers = lax.axis_size("worker")
    devices = workers * lax.axis_size("mp")
    me = lax.axis_index("worker")
    length = gradients.shape[1]
    rows = length // workers // LANES
    pieces = gradients.reshape(workers, rows, LANES)
    core = me & 1
    high, give, keep = split(core.reshape(1), pieces)
    columns = lax.all_to_all(high, "worker", split_axis=0, concat_axis=0, tiled=True)
    scale = 1.0 / float(neighbours.shape[1] * length * lax.axis_size("mp"))
    partial_value = partial_scores(neighbours, columns, devices, scale)
    everyone = lax.all_to_all(
        partial_value, ("worker", "mp"), split_axis=0, concat_axis=0, tiled=True
    )
    scores = jnp.sum(everyone, axis=0)[0, :workers]

    chips = workers // 2
    chip = me >> 1
    best = winner[0]
    got = lax.ppermute(give, "worker", [(i, i ^ 1) for i in range(workers)])
    mine = jnp.where((best & 1) == core, keep, got)
    low = lax.dynamic_index_in_dim(mine, chip, 0, keepdims=False)
    for d in range(1, chips):
        sent = lax.dynamic_index_in_dim(mine, chip ^ d, 0, keepdims=False)
        came = lax.ppermute(sent, "worker", [(i, i ^ (2 * d)) for i in range(workers)])
        low = jnp.where(best >> 1 == chip ^ d, came, low)
    rounded = lax.dynamic_index_in_dim(columns, best, 0, keepdims=False)
    aggregate = rounded.astype(jnp.float32) + low.astype(jnp.float32)
    return (scores, aggregate.reshape(-1))


def solution(mesh):
    in_specs = (P("worker", "mp"), P(), P())
    out_specs = (P(), P(("mp", "worker")))
    return jax.shard_map(body, mesh=mesh, in_specs=in_specs, out_specs=out_specs, check_vma=False)
```

```python
import jax
import jax.numpy as jnp
from jax import lax
from jax.experimental import pallas as pl
from jax.experimental.pallas import tpu as pltpu
from jax.sharding import PartitionSpec as P

LANES = 128


def on_chip(x):
    return pltpu.with_memory_space_constraint(x, pltpu.VMEM)


def exchange(x, step, workers):
    return lax.ppermute(x, "worker", [(i, i ^ step) for i in range(workers)])


def split(me, pieces):
    workers, rows, lanes = pieces.shape
    order = sorted(range(workers), key=lambda d: -d)

    def kernel(me_ref, pieces_ref, *refs):
        high, (give, keep, buffer, sems) = refs[:workers], refs[workers:]
        copies = {}
        for d in order:
            copies[d] = pltpu.make_async_copy(
                pieces_ref.at[me_ref[0] ^ d], buffer.at[d], sems.at[d]
            )
            copies[d].start()
        for d in order:
            copies[d].wait()
            value = buffer[d]
            rounded = value.astype(jnp.bfloat16)
            high[d][...] = rounded
            low = (value - rounded.astype(jnp.float32)).astype(jnp.bfloat16)
            (give if d & 1 else keep)[d >> 1] = low

    piece = pltpu.VMEM((rows, lanes), jnp.bfloat16)
    half = pltpu.VMEM((workers // 2, rows, lanes), jnp.bfloat16)
    return pl.pallas_call(
        kernel,
        out_shape=(piece,) * workers + (half, half),
        in_specs=[
            pl.BlockSpec(memory_space=pltpu.SMEM),
            pl.BlockSpec(memory_space=pl.ANY),
        ],
        out_specs=(pl.BlockSpec(memory_space=pltpu.VMEM),) * (workers + 2),
        scratch_shapes=[
            pltpu.VMEM((workers, rows, lanes), jnp.float32),
            pltpu.SemaphoreType.DMA((workers,)),
        ],
        name="split",
    )(me, pieces)


def partial_scores(counts, blocks, devices, scale):
    workers = len(blocks)
    rows, lanes = blocks[0].shape
    pairs = [(a, b) for a in range(workers) for b in range(a + 1, workers)]
    chunk = 16

    def kernel(counts_ref, *refs):
        blocks_ref, out = refs[:workers], refs[workers]

        def step(r, sums):
            at = pl.ds(pl.multiple_of(r * chunk, chunk), chunk)
            rows_of = [ref[at, :].astype(jnp.float32) for ref in blocks_ref]
            new = []
            for (a, b), total in zip(pairs, sums):
                diff = rows_of[a] - rows_of[b]
                square = diff * diff
                new.append(total + square[:8] + square[8:])
            return tuple(new)

        zero = jnp.zeros((8, lanes), jnp.float32)
        sums = lax.fori_loop(0, rows // chunk, step, (zero,) * len(pairs))
        lane = lax.broadcasted_iota(jnp.int32, (1, lanes), 1)
        row = jnp.zeros((1, lanes), jnp.float32)
        own = [zero] * workers
        for (a, b), total in zip(pairs, sums):
            own[a] = own[a] + counts_ref[a, b] * total
            own[b] = own[b] + counts_ref[b, a] * total
        me = counts_ref[workers, 0].astype(jnp.int32)
        for a in range(workers):
            total = jnp.sum(jnp.sum(own[a], axis=0, keepdims=True), axis=1, keepdims=True)
            row = jnp.where(lane == me ^ a, total * scale, row)
        out[...] = jnp.broadcast_to(row[None], out.shape)

    return pl.pallas_call(
        kernel,
        out_shape=pltpu.VMEM((devices, 1, LANES), jnp.float32),
        in_specs=[pl.BlockSpec(memory_space=pltpu.SMEM)]
        + [pl.BlockSpec(memory_space=pltpu.VMEM)] * workers,
        out_specs=pl.BlockSpec(memory_space=pltpu.VMEM),
        name="scores",
    )(counts, *blocks)


def merge(place, blocks, lows):
    workers = len(blocks)

    def kernel(place_ref, *refs):
        high, low, out = refs[:workers], refs[workers:-1], refs[-1]
        for d in range(workers):

            @pl.when(place_ref[0] == d)
            def _(d=d):
                out[...] = high[d][...].astype(jnp.float32) + low[d >> 1][...].astype(jnp.float32)

    return pl.pallas_call(
        kernel,
        out_shape=jax.ShapeDtypeStruct(blocks[0].shape, jnp.float32),
        in_specs=[pl.BlockSpec(memory_space=pltpu.SMEM)]
        + [pl.BlockSpec(memory_space=pltpu.VMEM)] * (workers + len(lows)),
        out_specs=pl.BlockSpec(memory_space=pltpu.VMEM),
        name="merge",
    )(place, *blocks, *lows)


def layer(gradients, neighbours, winner):
    workers = lax.axis_size("worker")
    devices = workers * lax.axis_size("mp")
    me = lax.axis_index("worker")
    length = gradients.shape[1]
    rows = length // workers // LANES
    pieces = gradients.reshape(workers, rows, LANES)
    parts = split(me.reshape(1), pieces)
    high, give, keep = parts[:workers], parts[workers], parts[workers + 1]
    blocks = [high[0]]
    for d in range(1, workers):
        blocks.append(exchange(high[d], d, workers))
    blocks = [on_chip(block) for block in blocks]

    place = winner ^ me
    got = exchange(give, 1, workers)
    mine = jnp.where((place[0] & 1) == 0, keep, got)
    lows = [mine[0]]
    for j in range(1, workers // 2):
        lows.append(exchange(mine[j], 2 * j, workers))
    lows = [on_chip(low) for low in lows]

    index = jnp.arange(workers, dtype=jnp.int32) ^ me
    named = (neighbours[:, :, None] == index[None, None, :]).astype(jnp.float32).sum(axis=1)
    mine_rows = (index[:, None] == jnp.arange(workers, dtype=jnp.int32)[None, :]).astype(jnp.float32)
    counts = (mine_rows[:, :, None] * named[None]).sum(axis=1)
    counts = jnp.concatenate([counts, jnp.full((1, workers), me.astype(jnp.float32))], axis=0)
    scale = 1.0 / float(neighbours.shape[1] * length * lax.axis_size("mp"))
    partial_value = partial_scores(counts, blocks, devices, scale)
    everyone = lax.all_to_all(
        partial_value, ("worker", "mp"), split_axis=0, concat_axis=0, tiled=True
    )
    scores = jnp.sum(everyone, axis=0)[0, :workers]
    aggregate = merge(place, blocks, lows)
    return (scores, aggregate.reshape(-1))


def solution(mesh):
    in_specs = (P("worker", "mp"), P(), P())
    out_specs = (P(), P(("mp", "worker")))
    return jax.shard_map(layer, mesh=mesh, in_specs=in_specs, out_specs=out_specs, check_vma=False)
```

```python
import jax
import jax.numpy as jnp
from jax import lax
from jax.experimental import pallas as pl
from jax.experimental.pallas import tpu as pltpu
from jax.sharding import PartitionSpec as P

LANES = 128


def on_chip(x):
    return pltpu.with_memory_space_constraint(x, pltpu.VMEM)


def exchange(x, step, workers):
    return lax.ppermute(x, "worker", [(i, i ^ step) for i in range(workers)])


def split(me, pieces):
    workers, rows, lanes = pieces.shape
    order = sorted(range(workers), key=lambda d: -d)

    def kernel(me_ref, pieces_ref, *refs):
        high, (give, keep, buffer, sems) = refs[:workers], refs[workers:]
        copies = {}
        for d in order:
            copies[d] = pltpu.make_async_copy(
                pieces_ref.at[me_ref[0] ^ d], buffer.at[d], sems.at[d]
            )
            copies[d].start()
        for d in order:
            copies[d].wait()
            value = buffer[d]
            rounded = value.astype(jnp.bfloat16)
            high[d][...] = rounded
            low = (value - rounded.astype(jnp.float32)).astype(jnp.bfloat16)
            (give if d & 1 else keep)[d >> 1] = low

    piece = pltpu.VMEM((rows, lanes), jnp.bfloat16)
    half = pltpu.VMEM((workers // 2, rows, lanes), jnp.bfloat16)
    return pl.pallas_call(
        kernel,
        out_shape=(piece,) * workers + (half, half),
        in_specs=[
            pl.BlockSpec(memory_space=pltpu.SMEM),
            pl.BlockSpec(memory_space=pl.ANY),
        ],
        out_specs=(pl.BlockSpec(memory_space=pltpu.VMEM),) * (workers + 2),
        scratch_shapes=[
            pltpu.VMEM((workers, rows, lanes), jnp.float32),
            pltpu.SemaphoreType.DMA((workers,)),
        ],
        name="split",
    )(me, pieces)


def partial_scores(weights, blocks, devices):
    workers = len(blocks)
    rows, lanes = blocks[0].shape
    pairs = [(a, b) for a in range(workers) for b in range(a + 1, workers)]
    chunk = 16

    def kernel(weights_ref, *refs):
        blocks_ref, out = refs[:workers], refs[workers]

        def step(r, sums):
            at = pl.ds(pl.multiple_of(r * chunk, chunk), chunk)
            rows_of = [ref[at, :].astype(jnp.float32) for ref in blocks_ref]
            new = []
            for (a, b), total in zip(pairs, sums):
                diff = rows_of[a] - rows_of[b]
                square = diff * diff
                new.append(total + square[:8] + square[8:])
            return tuple(new)

        zero = jnp.zeros((8, lanes), jnp.float32)
        sums = lax.fori_loop(0, rows // chunk, step, (zero,) * len(pairs))
        own = [zero] * workers
        for (a, b), total in zip(pairs, sums):
            own[a] = own[a] + weights_ref[a * workers + b][None] * total
            own[b] = own[b] + weights_ref[b * workers + a][None] * total
        row = jnp.zeros((1, lanes), jnp.float32)
        for a in range(workers):
            total = jnp.sum(jnp.sum(own[a], axis=0, keepdims=True), axis=1, keepdims=True)
            row = row + total * weights_ref[workers * workers + a][None]
        out[...] = jnp.broadcast_to(row[None], out.shape)

    return pl.pallas_call(
        kernel,
        out_shape=pltpu.VMEM((devices, 1, LANES), jnp.float32),
        in_specs=[pl.BlockSpec(memory_space=pltpu.VMEM)] * (workers + 1),
        out_specs=pl.BlockSpec(memory_space=pltpu.VMEM),
        name="scores",
    )(weights, *blocks)


def merge(place, blocks, lows):
    workers = len(blocks)

    def kernel(place_ref, *refs):
        high, low, out = refs[:workers], refs[workers:-1], refs[-1]
        for d in range(workers):

            @pl.when(place_ref[0] == d)
            def _(d=d):
                out[...] = high[d][...].astype(jnp.float32) + low[d >> 1][...].astype(jnp.float32)

    return pl.pallas_call(
        kernel,
        out_shape=jax.ShapeDtypeStruct(blocks[0].shape, jnp.float32),
        in_specs=[pl.BlockSpec(memory_space=pltpu.SMEM)]
        + [pl.BlockSpec(memory_space=pltpu.VMEM)] * (workers + len(lows)),
        out_specs=pl.BlockSpec(memory_space=pltpu.VMEM),
        name="merge",
    )(place, *blocks, *lows)


def layer(gradients, neighbours, winner):
    workers = lax.axis_size("worker")
    devices = workers * lax.axis_size("mp")
    me = lax.axis_index("worker")
    length = gradients.shape[1]
    rows = length // workers // LANES
    pieces = gradients.reshape(workers, rows, LANES)
    parts = split(me.reshape(1), pieces)
    high, give, keep = parts[:workers], parts[workers], parts[workers + 1]
    blocks = [high[0]]
    for d in range(1, workers):
        blocks.append(exchange(high[d], d, workers))
    blocks = [on_chip(block) for block in blocks]

    place = winner ^ me
    got = exchange(give, 1, workers)
    mine = jnp.where((place[0] & 1) == 0, keep, got)
    lows = [mine[0]]
    for j in range(1, workers // 2):
        lows.append(exchange(mine[j], 2 * j, workers))
    lows = [on_chip(low) for low in lows]

    scale = 1.0 / float(neighbours.shape[1] * length * lax.axis_size("mp"))
    index = jnp.arange(workers, dtype=jnp.int32) ^ me
    named = (neighbours[:, :, None] == index[None, None, :]).astype(jnp.float32).sum(axis=1)
    is_row = (index[:, None] == jnp.arange(workers, dtype=jnp.int32)[None, :]).astype(jnp.float32)
    counts = (is_row[:, :, None] * named[None]).sum(axis=1).reshape(-1, 1)
    lane = jnp.arange(LANES, dtype=jnp.int32)[None, :]
    places = jnp.where(lane == index[:, None], jnp.float32(scale), jnp.float32(0.0))
    weights = jnp.concatenate([jnp.broadcast_to(counts, (workers * workers, LANES)), places])
    partial_value = partial_scores(on_chip(weights), blocks, devices)
    everyone = lax.all_to_all(
        partial_value, ("worker", "mp"), split_axis=0, concat_axis=0, tiled=True
    )
    scores = jnp.sum(everyone, axis=0)[0, :workers]
    aggregate = merge(place, blocks, lows)
    return (scores, aggregate.reshape(-1))


def solution(mesh):
    in_specs = (P("worker", "mp"), P(), P())
    out_specs = (P(), P(("mp", "worker")))
    return jax.shard_map(layer, mesh=mesh, in_specs=in_specs, out_specs=out_specs, check_vma=False)
```

```python
import jax
import jax.numpy as jnp
from jax import lax
from jax.experimental import pallas as pl
from jax.experimental.pallas import tpu as pltpu
from jax.sharding import PartitionSpec as P

LANES = 128


def on_chip(x):
    return pltpu.with_memory_space_constraint(x, pltpu.VMEM)


def exchange(x, step, workers):
    return lax.ppermute(x, "worker", [(i, i ^ step) for i in range(workers)])


def split(me, pieces, wanted, remainder):
    workers, rows, lanes = pieces.shape
    order = sorted(range(workers) if remainder else wanted, key=lambda d: (d not in wanted, -d))

    def kernel(me_ref, pieces_ref, *refs):
        high = dict(zip(wanted, refs))
        low_refs, (buffer, sems) = refs[len(wanted):-2], refs[-2:]
        copies = {}
        for n, d in enumerate(order):
            copies[d] = pltpu.make_async_copy(
                pieces_ref.at[me_ref[0] ^ d], buffer.at[n], sems.at[n]
            )
            copies[d].start()
        for n, d in enumerate(order):
            copies[d].wait()
            value = buffer[n]
            rounded = value.astype(jnp.bfloat16)
            if d in wanted:
                high[d][...] = rounded
            if remainder:
                low = (value - rounded.astype(jnp.float32)).astype(jnp.bfloat16)
                low_refs[d & 1][d >> 1] = low

    piece = pltpu.VMEM((rows, lanes), jnp.bfloat16)
    half = pltpu.VMEM((workers // 2, rows, lanes), jnp.bfloat16)
    out_shape = (piece,) * len(wanted) + ((half, half) if remainder else ())
    return pl.pallas_call(
        kernel,
        out_shape=out_shape,
        in_specs=[
            pl.BlockSpec(memory_space=pltpu.SMEM),
            pl.BlockSpec(memory_space=pl.ANY),
        ],
        out_specs=(pl.BlockSpec(memory_space=pltpu.VMEM),) * len(out_shape),
        scratch_shapes=[
            pltpu.VMEM((len(order), rows, lanes), jnp.float32),
            pltpu.SemaphoreType.DMA((len(order),)),
        ],
    )(me, pieces)


def partial_scores(weights, blocks, devices):
    workers = len(blocks)
    rows, lanes = blocks[0].shape
    pairs = [(a, b) for a in range(workers) for b in range(a + 1, workers)]
    chunk = 16

    def kernel(weights_ref, *refs):
        blocks_ref, out = refs[:workers], refs[workers]

        def step(r, sums):
            at = pl.ds(pl.multiple_of(r * chunk, chunk), chunk)
            rows_of = [ref[at, :].astype(jnp.float32) for ref in blocks_ref]
            new = []
            for (a, b), total in zip(pairs, sums):
                diff = rows_of[a] - rows_of[b]
                square = diff * diff
                new.append(total + square[:8] + square[8:])
            return tuple(new)

        zero = jnp.zeros((8, lanes), jnp.float32)
        sums = lax.fori_loop(0, rows // chunk, step, (zero,) * len(pairs), unroll=2)
        own = [zero] * workers
        for (a, b), total in zip(pairs, sums):
            own[a] = own[a] + weights_ref[a * workers + b][None] * total
            own[b] = own[b] + weights_ref[b * workers + a][None] * total
        row = jnp.zeros((1, lanes), jnp.float32)
        for a in range(workers):
            total = jnp.sum(jnp.sum(own[a], axis=0, keepdims=True), axis=1, keepdims=True)
            row = row + total * weights_ref[workers * workers + a][None]
        out[...] = jnp.broadcast_to(row[None], out.shape)

    return pl.pallas_call(
        kernel,
        out_shape=pltpu.VMEM((devices, 1, LANES), jnp.float32),
        in_specs=[pl.BlockSpec(memory_space=pltpu.VMEM)] * (workers + 1),
        out_specs=pl.BlockSpec(memory_space=pltpu.VMEM),
        name="scores",
    )(weights, *blocks)


def merge(place, blocks, lows):
    workers = len(blocks)

    def kernel(place_ref, *refs):
        high, low, out = refs[:workers], refs[workers:-1], refs[-1]
        for d in range(workers):

            @pl.when(place_ref[0] == d)
            def _(d=d):
                out[...] = high[d][...].astype(jnp.float32) + low[d >> 1][...].astype(jnp.float32)

    return pl.pallas_call(
        kernel,
        out_shape=jax.ShapeDtypeStruct(blocks[0].shape, jnp.float32),
        in_specs=[pl.BlockSpec(memory_space=pltpu.SMEM)]
        + [pl.BlockSpec(memory_space=pltpu.VMEM)] * (workers + len(lows)),
        out_specs=pl.BlockSpec(memory_space=pltpu.VMEM),
        name="merge",
    )(place, *blocks, *lows)


def layer(gradients, neighbours, winner):
    workers = lax.axis_size("worker")
    devices = workers * lax.axis_size("mp")
    me = lax.axis_index("worker")
    length = gradients.shape[1]
    rows = length // workers // LANES
    pieces = gradients.reshape(workers, rows, LANES)
    first = list(range(2, workers, 2))
    others = [d for d in range(workers) if d not in first]
    high = dict(zip(first, split(me.reshape(1), pieces, first, False)))
    *parts, keep, give = split(me.reshape(1), pieces, others, True)
    high.update(zip(others, parts))
    blocks = [high[0]]
    for d in range(1, workers):
        blocks.append(exchange(high[d], d, workers))
    blocks = [on_chip(block) for block in blocks]

    place = winner ^ me
    got = exchange(give, 1, workers)
    mine = jnp.where((place[0] & 1) == 0, keep, got)
    lows = [mine[0]]
    for j in range(1, workers // 2):
        lows.append(exchange(mine[j], 2 * j, workers))
    lows = [on_chip(low) for low in lows]

    scale = 1.0 / float(neighbours.shape[1] * length * lax.axis_size("mp"))
    index = jnp.arange(workers, dtype=jnp.int32) ^ me
    named = (neighbours[:, :, None] == index[None, None, :]).astype(jnp.float32).sum(axis=1)
    is_row = (index[:, None] == jnp.arange(workers, dtype=jnp.int32)[None, :]).astype(jnp.float32)
    counts = (is_row[:, :, None] * named[None]).sum(axis=1).reshape(-1, 1)
    lane = jnp.arange(LANES, dtype=jnp.int32)[None, :]
    places = jnp.where(lane == index[:, None], jnp.float32(scale), jnp.float32(0.0))
    weights = jnp.concatenate([jnp.broadcast_to(counts, (workers * workers, LANES)), places])
    partial_value = partial_scores(on_chip(weights), blocks, devices)
    everyone = lax.all_to_all(
        partial_value, ("worker", "mp"), split_axis=0, concat_axis=0, tiled=True
    )
    scores = jnp.sum(everyone, axis=0)[0, :workers]
    aggregate = merge(place, blocks, lows)
    return (scores, aggregate.reshape(-1))


def solution(mesh):
    in_specs = (P("worker", "mp"), P(), P())
    out_specs = (P(), P(("mp", "worker")))
    return jax.shard_map(layer, mesh=mesh, in_specs=in_specs, out_specs=out_specs, check_vma=False)
```
